32 devices in a mesh: blk: 32 (over z, y, x, core).
Axes of the slice: x: 2, y: 2, z: 4, core: 2. Of those that a mesh axis runs over, the one named last changes fastest.
Arguments:
- tiles: float32 [128, 3, 256, 256], P('blk'), may hold values from -0.109375 to 0.109375
- offsets: int32 [128, 3], P('blk'), may hold values from -2 to 2, as said below
- start: float32 [32768, 128], P('blk'), may hold values from -6 to 6
Outputs:
- grams: float32 [2, 8, 8, 128], replicated
- final: float32 [32768, 128], P('blk')
The draws below stay inside these ranges and needn't reach their ends.
Inputs may be any that keep to these rules, and one draw needn't show every extreme that they name: The 3 offsets of a block row are all different.
All inputs are finite; a program needn't handle non-finite values.
Results may differ from the reference program's by a relative error of at most 0.00018.
Values sent between devices are 32-bit elements; how exact they have to be, the bound alone decides.
A program may use at most 128 MiB of HBM per device.

```python
import jax
import jax.numpy as jnp
from jax import lax

TILE = 256
SLOTS = 3
REACH = 2
PROBES = 128
OUTER = 2
DEPTH = 4
NBLK = 128
NROWS = 32768


def draw_offsets(key, part):
    width = 2 * REACH + 1
    scores = jax.random.randint(key, (NBLK, width), 0, 1 << 20) * width + jnp.arange(width, dtype=jnp.int32)
    order = jnp.argsort(scores, axis=1)
    return (order[:, :SLOTS] - REACH).astype(jnp.int32)


def shard_levels(own_key, extent, cuts, low, largest):
    gain = 1.0
    for dim, blocks in cuts:
        steps = jax.random.uniform(jax.random.fold_in(jax.random.fold_in(own_key, 6), dim), (blocks,), jnp.float32, low / len(cuts), largest / len(cuts))
        gain = gain * jnp.repeat(jnp.exp(steps), extent[dim] // blocks).reshape((-1,) + (1,) * (len(extent) - 1 - dim))
    return gain


def normal_values(key, dims, deviation, most, pieces=(), kind=jnp.bfloat16):
    entries = jax.random.normal(key, dims, jnp.float32) * deviation
    if len(pieces) > 0:
        entries = shard_levels(key, dims, pieces, -0.22, 0.18) * entries
    return jnp.clip(entries, min=-most, max=most).astype(kind)


def setup_inputs(seed: int = 0) -> dict:
    key_list = jax.random.split(jax.random.key(seed), 4)
    return {
        "tiles": normal_values(key_list[0], (NBLK, SLOTS, TILE, TILE), (4 * SLOTS * TILE) ** -0.5, 0.109375, ((0, 32),), jnp.float32),
        "offsets": draw_offsets(jax.random.fold_in(key_list[3], 71), 0),
        "start": normal_values(key_list[2], (NROWS, PROBES), 1.0, 6.0, ((0, 32),), jnp.float32),
    }


def forward_all(tiles, offsets, field):
    nblk = tiles.shape[0]
    blocks = field.reshape(nblk, TILE, field.shape[1])
    index = (jnp.arange(nblk, dtype=jnp.int32)[:, None] + offsets) % nblk
    picked = blocks[index]
    image = jnp.einsum('rkab,rkbp->rap', tiles, picked, precision=lax.Precision.HIGHEST)
    return image.reshape(field.shape)

def adjoint_all(tiles, offsets, field):
    nblk = tiles.shape[0]
    probes = field.shape[1]
    blocks = field.reshape(nblk, TILE, probes)
    parts = jnp.einsum('rkab,rap->rkbp', tiles, blocks, precision=lax.Precision.HIGHEST)
    target = ((jnp.arange(nblk, dtype=jnp.int32)[:, None] + offsets) % nblk).reshape(-1)
    total = jnp.zeros_like(blocks).at[target].add(parts.reshape(-1, TILE, probes))
    return total.reshape(field.shape)

def reference(tiles, offsets, start):
    current = start
    grams = []
    for outer in range(OUTER):
        basis_p = [current]
        basis_q = []
        for depth in range(DEPTH):
            image = forward_all(tiles, offsets, basis_p[-1])
            basis_q.append(image)
            basis_p.append(adjoint_all(tiles, offsets, image))
        stack = jnp.stack(basis_p[:DEPTH] + basis_q)
        gram = jnp.einsum('arp,brp->abp', stack, stack, precision=lax.Precision.HIGHEST) / NROWS
        grams.append(gram)
        current = basis_p[DEPTH] / jnp.sqrt(gram[-1, -1] + 0.25)
    return (jnp.stack(grams), current)
```

```python
import functools

import jax
import jax.numpy as jnp
from jax import lax
from jax.experimental import pallas as pl
from jax.experimental.pallas import tpu as pltpu
from jax.sharding import PartitionSpec as P

REACH = 2
OUTER = 2
DEPTH = 4
SIZE = 2 * DEPTH
STREAMS = 2
FIRST = [0, 1, 3, 5, 8, 11, 16, 20]
GROUPS = [(0, 8), (8, 8), (16, 16)]
CLOSES = [3, 5, 7]
GAUGE = 3
GROWTH = 2.0 ** (14 * (SIZE - 1 - GAUGE))
MESH = pl.DeviceIdType.MESH
F32 = jnp.float32
BF16 = jnp.bfloat16


def halves(x):
    high = x.astype(BF16)
    return high, (x - high.astype(F32)).astype(BF16)


def kernel(
    n,
    stages,
    total_rows,
    off_ref,
    tiles_hbm,
    start_hbm,
    gram_ref,
    final_ref,
    raw,
    first,
    fwd_high,
    fwd_low,
    adj_high,
    adj_low,
    basis,
    field,
    image,
    parts,
    acc,
    halo,
    give,
    got,
    scale,
    gacc,
    grow,
    box_a,
    box_b,
    box_c,
    totals,
    load_sem,
    acc_send,
    acc_recv,
    part_send,
    part_recv,
    sum_send,
    sum_recv,
):
    nblk, slots, tile, _ = raw.shape
    streams = basis.shape[0]
    width = basis.shape[3]
    probes = streams * width
    last_pair = OUTER * DEPTH - 1
    me = lax.axis_index("blk")
    slow = lax.rem(me, 2)
    fast = 1 - slow

    load_start = pltpu.make_async_copy(start_hbm, first, load_sem.at[0])
    load_start.start()
    load_tiles = pltpu.make_async_copy(tiles_hbm, raw, load_sem.at[1])
    load_tiles.start()

    barrier = pltpu.get_barrier_semaphore()

    def bit(b):
        return lax.rem(me // (1 << b), 2)

    def flipped(st, mask):
        other = me
        for m, b in enumerate(stages[st]):
            if mask >> m & 1:
                other = other + (1 << b) * (1 - 2 * bit(b))
        return other

    def masks(st):
        return range(1, 1 << len(stages[st]))

    others = [lax.rem(me + n - 1, n), lax.rem(me + 1, n)]
    others += [flipped(st, mask) for st in range(len(stages)) for mask in masks(st)]
    for other in others:
        pl.semaphore_signal(barrier, inc=1, device_id=(other,), device_id_type=MESH)

    def block(side, k):
        return side * (nblk - 1) + k * (1 - 2 * side)

    def beyond(side, k):
        return side * (nblk + 1 + 2 * k) - 1 - k

    def neighbour(side):
        return (lax.rem(me + n - 1 + 2 * side, n),)

    def acc_copy(slot, s, side, k, there):
        return pltpu.make_async_remote_copy(
            src_ref=acc.at[s, block(side, k)],
            dst_ref=halo.at[slot, s, there, k],
            send_sem=acc_send.at[slot, s, side, k],
            recv_sem=acc_recv.at[slot, s, there, k],
            device_id=neighbour(side),
            device_id_type=MESH,
        )

    def part_copy(slot, s, side, k, there):
        return pltpu.make_async_remote_copy(
            src_ref=give.at[s, side, k],
            dst_ref=got.at[slot, s, there, k],
            send_sem=part_send.at[slot, s, side, k],
            recv_sem=part_recv.at[slot, s, there, k],
            device_id=neighbour(side),
            device_id_type=MESH,
        )

    boxes = [box_a, box_b, box_c]

    def place(st):
        return sum(bit(b) << m for m, b in enumerate(stages[st]))

    def stage_copy(o, kind, st, mask):
        return pltpu.make_async_remote_copy(
            src_ref=boxes[kind].at[o, st, place(st)],
            dst_ref=boxes[kind].at[o, st, place(st)],
            send_sem=sum_send.at[o, kind, st, mask - 1],
            recv_sem=sum_recv.at[o, kind, st, mask - 1],
            device_id=(flipped(st, mask),),
            device_id_type=MESH,
        )

    def stage_open(o, kind, st, value):
        boxes[kind][o, st, place(st)] = value
        for mask in masks(st):
            stage_copy(o, kind, st, mask).start()

    def group_open(o, kind):
        begin, count = GROUPS[kind]
        stage_open(o, kind, 0, grow[o, pl.ds(begin, count)])

    def advance(o, kind, st):
        for mask in masks(st):
            stage_copy(o, kind, st, mask).wait()
        value = boxes[kind][o, st, 0]
        for m in masks(st):
            value = value + boxes[kind][o, st, m]
        if st + 1 < len(stages):
            stage_open(o, kind, st + 1, value)
        else:
            begin, count = GROUPS[kind]
            totals[o, pl.ds(begin, count)] = value

    lap = streams * DEPTH
    agenda = {}
    taken = {}
    for o, kind, whens in [
        (0, 0, [2 * streams]),
        (0, 1, [3 * streams, 4 * streams]),
        (0, 2, [5 * streams - 1, 5 * streams + 1]),
        (1, 0, [lap + 2 * streams, lap + 3 * streams]),
        (1, 1, [lap + 3 * streams, lap + 4 * streams - 1]),
        (1, 2, []),
    ]:
        for st, when in enumerate(whens[: len(stages)]):
            agenda.setdefault(when, []).append((o, kind, st))
        taken[o, kind] = min(len(whens), len(stages))

    def point(at):
        for when, steps in agenda.items():

            @pl.when(at == when)
            def _():
                for step in steps:
                    advance(*step)

    def finish(o, kind):
        for st in range(taken[o, kind], len(stages)):
            advance(o, kind, st)

    def ranks(i):
        offs = [off_ref[i, k] for k in range(slots)]
        return offs, [
            sum((offs[m] < offs[k]).astype(jnp.int32) for m in range(slots) if m != k)
            for k in range(slots)
        ]

    def sorted_slot(i, s):
        offs, rank = ranks(i)
        index, off = 0, 0
        for k in range(slots):
            index = jnp.where(rank[k] == s, k, index)
            off = jnp.where(rank[k] == s, offs[k], off)
        return index, off

    def source(i, d):
        offs, rank = ranks(i)
        index = nblk * slots
        for k in range(slots):
            index = jnp.where(offs[k] == d, i * slots + rank[k], index)
        return index

    def keep(ref, where, value):
        high, low = halves(value)
        ref[where + (pl.ds(0, width),)] = high
        ref[where + (pl.ds(width, width),)] = low

    def product(lhs, high, low):
        top = jnp.dot(lhs, high, preferred_element_type=F32)
        bottom = jnp.dot(lhs[:width], low, preferred_element_type=F32)
        return top[:width] + (top[width:] + bottom)

    def forward(s, i, begin, count):
        lhs = jnp.concatenate(
            [field[s, i + REACH + sorted_slot(i, begin + m)[1]] for m in range(count)], axis=1
        )
        span = pl.ds(pl.multiple_of(begin * tile, tile), count * tile)
        return product(lhs, fwd_high[i, span], fwd_low[i, span])

    def adjoint(s, i, begin, count):
        for m in range(count):
            k = begin + m
            parts[i * slots + k] = product(image[s, i], adj_high[i, k], adj_low[i, k])

    def edge(side, k):
        return side * (slots - REACH + k), REACH - k

    def inner(side, k):
        return (1 - side) * (REACH - k), slots - REACH + k

    middle = list(range(REACH, nblk - REACH))

    def rows_of(tl):
        return 1 + (tl + 1) // 2

    def first_row(tl):
        at = 0
        for t in range(1, SIZE):
            at = at + (FIRST[t] - FIRST[t - 1]) * (tl >= t)
        return at

    def gram_rows(o, tl, s):
        base = o * SIZE

        def one(v, carry):
            u = jnp.where(v == 0, tl, 2 * v - 1 - lax.rem(tl, 2))
            total = basis[s, base + tl, 0] * basis[s, base + u, 0]
            for i in range(1, nblk):
                total = total + basis[s, base + tl, i] * basis[s, base + u, i]
            lanes = total[:, :128]
            for c in range(128, tile, 128):
                lanes = lanes + total[:, c : c + 128]
            gacc[lax.rem(tl, 2), v, s] = lanes
            return carry

        lax.fori_loop(0, rows_of(tl), one, 0)

    def gram_close(o, tl):
        begin = first_row(tl)

        def one(v, carry):
            m = gacc[lax.rem(tl, 2), v].reshape(probes, 128).T
            grow[o, pl.ds(begin + v, 1), :] = jnp.sum(m, axis=0, keepdims=True)
            return carry

        lax.fori_loop(0, rows_of(tl), one, 0)
        for kind, last in enumerate(CLOSES):

            @pl.when(tl == last)
            def _():
                group_open(o, kind)

    def provisional(o):
        row = FIRST[GAUGE]
        return 1.0 / jnp.sqrt(totals[o, row : row + 1, :] / total_rows * GROWTH + 0.25)

    def gram(o, tl, s):
        gram_rows(o, tl, s)
        pl.when(s == streams - 1)(functools.partial(gram_close, o, tl))

    def phase(g, s):
        o, tl = g // DEPTH, 2 * lax.rem(g, DEPTH)
        t, slot = 2 * g, lax.rem(g, 2)
        which = ((tl == 0) & (g > 0)).astype(jnp.int32)

        @pl.when((s == 0) & (which == 1))
        def _():
            finish(0, 0)
            full = jnp.broadcast_to(provisional(0), (128, probes)).T
            for m in range(streams):
                for c in range(0, tile, 128):
                    scale[1, m, :, pl.ds(c, 128)] = full[m * width : (m + 1) * width]

        factor = scale[which, s]
        for i in middle:
            p = acc[s, i] * factor
            basis[s, t, i] = p
            keep(field, (s, i + REACH), p)
        for side in (fast, slow):
            for k in range(REACH):
                acc_copy(slot, s, side, k, side).wait()

                @pl.when(g > 0)
                def _():
                    part_copy(slot, s, side, k, side).wait()

                i = block(side, k)
                p = (acc[s, i] + got[slot, s, side, k]) * factor
                basis[s, t, i] = p
                keep(field, (s, i + REACH), p)
                beside = (halo[slot, s, side, k] + give[s, side, k]) * factor
                keep(field, (s, beyond(side, k) + REACH), beside)
            if side is fast:
                partial = [forward(s, block(fast, k), *edge(fast, k)) for k in range(REACH)]

        def image_row(i, q):
            basis[s, t + 1, i] = q
            keep(image, (s, i), q)

        def hand_over(side):
            for k in range(REACH):
                total = None
                for r in range(REACH - k):
                    term = parts[source(block(side, r), (2 * side - 1) * (r + 1 + k))]
                    total = term if total is None else total + term
                give[s, side, k] = total
                part_copy(1 - slot, s, side, k, 1 - side).start()

        for k in range(REACH):
            i = block(slow, k)
            image_row(i, forward(s, i, 0, slots))
        for k in range(REACH):
            i = block(fast, k)
            image_row(i, partial[k] + forward(s, i, *inner(fast, k)))
        for i in middle:
            image_row(i, forward(s, i, 0, slots))

        @pl.when(g == last_pair)
        def _():
            gram(o, tl, s)
            gram(o, tl + 1, s)

        for k in range(REACH):
            adjoint(s, block(slow, k), *edge(slow, k))
        hand_over(slow)
        for k in range(REACH):
            adjoint(s, block(slow, k), *inner(slow, k))
            adjoint(s, block(fast, k), 0, slots)
        for i in middle:
            adjoint(s, i, 0, slots)
        for i in range(nblk):
            total = None
            for r in range(nblk):
                if abs(i - r) <= REACH:
                    term = parts[source(r, i - r)]
                    total = term if total is None else total + term
            acc[s, i] = total

        @pl.when(g < last_pair)
        def _():
            for k in range(REACH):
                acc_copy(1 - slot, s, slow, k, 1 - slow).start()

        hand_over(fast)

        @pl.when(g < last_pair)
        def _():
            for k in range(REACH):
                acc_copy(1 - slot, s, fast, k, 1 - fast).start()
            gram(o, tl, s)
            gram(o, tl + 1, s)

        point(streams * g + s)

    grow[...] = jnp.zeros_like(grow)
    parts[nblk * slots] = jnp.zeros((width, tile), F32)
    scale[...] = jnp.ones_like(scale)
    give[...] = jnp.zeros_like(give)
    got[0] = jnp.zeros_like(got[0])
    load_start.wait()

    def turn(i):
        value = first[i].T
        for s in range(streams):
            acc[s, i] = value[s * width : (s + 1) * width]

    for k in range(REACH):
        turn(block(slow, k))
    pl.semaphore_wait(barrier, len(others))
    for s in range(streams):
        for k in range(REACH):
            acc_copy(0, s, slow, k, 1 - slow).start()
    for k in range(REACH):
        turn(block(fast, k))
    for s in range(streams):
        for k in range(REACH):
            acc_copy(0, s, fast, k, 1 - fast).start()
    for i in middle:
        turn(i)
    load_tiles.wait()

    def prepare(i, carry):
        for s in range(slots):
            value = raw[i, sorted_slot(i, s)[0]]
            high, low = halves(value)
            adj_high[i, s] = high
            adj_low[i, s] = low
            high, low = halves(value.T)
            fwd_high[i, pl.ds(s * tile, tile)] = high
            fwd_low[i, pl.ds(s * tile, tile)] = low
        return carry

    lax.fori_loop(0, nblk, prepare, 0)

    def pair(g, carry):
        def stream(s, c):
            phase(g, s)
            return c

        return lax.fori_loop(0, streams, stream, carry)

    lax.fori_loop(0, last_pair + 1, pair, 0)

    def last(s):
        slot = (last_pair + 1) % 2
        for side in (fast, slow):
            for k in range(REACH):
                i = block(side, k)
                part_copy(slot, s, side, k, side).wait()
                acc[s, i] += got[slot, s, side, k]

    for s in range(streams):
        last(s)

    for kind in range(len(GROUPS)):
        finish(OUTER - 1, kind)
    if OUTER > 1:
        for kind in range(1, len(GROUPS)):
            finish(0, kind)
    true = jnp.ones((1, probes), F32)
    for o in range(OUTER):
        for a in range(SIZE):
            for b in range(SIZE):
                x, y = a % DEPTH, b % DEPTH
                if a // DEPTH == b // DEPTH:
                    row = FIRST[x + y + a // DEPTH]
                else:
                    x, y = (x, y) if a < DEPTH else (y, x)
                    row = FIRST[2 * y + 1] + 1 + x if x <= y else FIRST[2 * x] + 1 + y
                value = totals[o, row : row + 1, :] / total_rows
                gram_ref[o, pl.ds(a * SIZE + b, 1), :] = value * true * true
        row = FIRST[SIZE - 1]
        corner = totals[o, row : row + 1, :] / total_rows * true * true
        norm = true / jnp.sqrt(corner + 0.25)
        if o < OUTER - 1:
            true = norm / provisional(o)
    for i in range(nblk):
        value = jnp.concatenate([acc[s, i] for s in range(streams)], axis=0)
        final_ref[i] = value.T * norm


def on_device(tiles, offsets, start):
    n = lax.axis_size("blk")
    levels = n.bit_length() - 1
    assert n == 1 << levels
    bits = [[0, 3, 4], [1, 2]] + [[b, b + 1] for b in range(5, levels, 2)]
    stages = [kept for group in bits if (kept := [b for b in group if b < levels])]
    nblk, slots, tile, _ = tiles.shape
    rows, probes = start.shape
    assert nblk >= 2 * REACH and slots >= REACH and OUTER == 2
    streams = STREAMS
    width = probes // streams
    dma = pltpu.SemaphoreType.DMA
    wide = (nblk, slots * tile, tile)
    square = (nblk, slots, tile, tile)
    grams, final = pl.pallas_call(
        functools.partial(kernel, n, stages, float(rows * n)),
        out_shape=(
            jax.ShapeDtypeStruct((OUTER, SIZE * SIZE, probes), F32),
            jax.ShapeDtypeStruct((nblk, tile, probes), F32),
        ),
        in_specs=[
            pl.BlockSpec(memory_space=pltpu.SMEM),
            pl.BlockSpec(memory_space=pl.ANY),
            pl.BlockSpec(memory_space=pl.ANY),
        ],
        out_specs=(pl.BlockSpec(memory_space=pltpu.VMEM), pl.BlockSpec(memory_space=pltpu.VMEM)),
        scratch_shapes=[
            pltpu.VMEM(tiles.shape, F32),
            pltpu.VMEM((nblk, tile, probes), F32),
            pltpu.VMEM(wide, BF16),
            pltpu.VMEM(wide, BF16),
            pltpu.VMEM(square, BF16),
            pltpu.VMEM(square, BF16),
            pltpu.VMEM((streams, OUTER * SIZE, nblk, width, tile), F32),
            pltpu.VMEM((streams, nblk + 2 * REACH, 2 * width, tile), BF16),
            pltpu.VMEM((streams, nblk, 2 * width, tile), BF16),
            pltpu.VMEM((nblk * slots + 1, width, tile), F32),
            pltpu.VMEM((streams, nblk, width, tile), F32),
            pltpu.VMEM((2, streams, 2, REACH, width, tile), F32),
            pltpu.VMEM((streams, 2, REACH, width, tile), F32),
            pltpu.VMEM((2, streams, 2, REACH, width, tile), F32),
            pltpu.VMEM((2, streams, width, tile), F32),
            pltpu.VMEM((2, 1 + DEPTH, streams, width, 128), F32),
            pltpu.VMEM((OUTER, 32, probes), F32),
        ]
        + [pltpu.VMEM((OUTER, len(stages), 8, count, probes), F32) for _, count in GROUPS]
        + [
            pltpu.VMEM((OUTER, 32, probes), F32),
            dma((2,)),
            dma((2, streams, 2, REACH)),
            dma((2, streams, 2, REACH)),
            dma((2, streams, 2, REACH)),
            dma((2, streams, 2, REACH)),
            dma((OUTER, len(GROUPS), len(stages), 7)),
            dma((OUTER, len(GROUPS), len(stages), 7)),
        ],
        compiler_params=pltpu.CompilerParams(collective_id=0, has_side_effects=True),
    )(offsets, tiles, start.reshape(nblk, tile, probes))
    return grams.reshape(OUTER, SIZE, SIZE, probes), final.reshape(rows, probes)


def solution(mesh):
    placed = (P("blk", None, None, None), P("blk", None), P("blk", None))
    return jax.shard_map(
        on_device, mesh=mesh, in_specs=placed, out_specs=(P(), P("blk", None)), check_vma=False
    )
```

```python
import functools

import jax
import jax.numpy as jnp
from jax import lax
from jax.experimental import pallas as pl
from jax.experimental.pallas import tpu as pltpu
from jax.sharding import PartitionSpec as P

REACH = 2
OUTER = 2
DEPTH = 4
SIZE = 2 * DEPTH
STREAMS = 2
FIRST = [0, 1, 3, 5, 8, 11, 15, 24]
GROUPS = [(0, 8), (8, 16), (24, 8)]
CLOSES = [3, 6, 7]
GAUGE = 3
GROWTH = 2.0 ** (14 * (SIZE - 1 - GAUGE))
MESH = pl.DeviceIdType.MESH
F32 = jnp.float32
BF16 = jnp.bfloat16


def halves(x):
    high = x.astype(BF16)
    return high, (x - high.astype(F32)).astype(BF16)


def provisional(totals, o, total_rows):
    row = FIRST[GAUGE]
    return 1.0 / jnp.sqrt(totals[o, row : row + 1, :] / total_rows * GROWTH + 0.25)


def kernel(
    n,
    stages,
    total_rows,
    off_hbm,
    tiles_hbm,
    start_hbm,
    totals,
    ends,
    off_ref,
    raw,
    first,
    fwd_high,
    fwd_low,
    adj_high,
    adj_low,
    basis,
    field,
    image,
    parts,
    acc,
    halo,
    give,
    got,
    scale,
    gacc,
    grow,
    box_a,
    box_b,
    box_c,
    load_sem,
    acc_send,
    acc_recv,
    part_send,
    part_recv,
    sum_send,
    sum_recv,
):
    nblk, slots, tile, _ = raw.shape
    streams = basis.shape[0]
    width = basis.shape[3]
    probes = streams * width
    last_pair = OUTER * DEPTH - 1
    me = lax.axis_index("blk")
    slow = lax.rem(me, 2)
    fast = 1 - slow

    load_start = pltpu.make_async_copy(start_hbm, first, load_sem.at[0])
    load_start.start()
    load_tiles = pltpu.make_async_copy(tiles_hbm, raw, load_sem.at[1])
    load_tiles.start()
    load_offs = pltpu.make_async_copy(off_hbm, off_ref, load_sem.at[2])
    load_offs.start()

    barrier = pltpu.get_barrier_semaphore()

    def bit(b):
        return lax.rem(me // (1 << b), 2)

    def flipped(st, mask):
        other = me
        for m, b in enumerate(stages[st]):
            if mask >> m & 1:
                other = other + (1 << b) * (1 - 2 * bit(b))
        return other

    def masks(st):
        return range(1, 1 << len(stages[st]))

    others = [lax.rem(me + n - 1, n), lax.rem(me + 1, n)]
    others += [flipped(st, mask) for st in range(len(stages)) for mask in masks(st)]
    for other in others:
        pl.semaphore_signal(barrier, inc=1, device_id=(other,), device_id_type=MESH)

    def block(side, k):
        return side * (nblk - 1) + k * (1 - 2 * side)

    def beyond(side, k):
        return side * (nblk + 1 + 2 * k) - 1 - k

    def neighbour(side):
        return (lax.rem(me + n - 1 + 2 * side, n),)

    def acc_copy(slot, s, side, k, there):
        return pltpu.make_async_remote_copy(
            src_ref=acc.at[s, block(side, k)],
            dst_ref=halo.at[slot, s, there, k],
            send_sem=acc_send.at[slot, s, side, k],
            recv_sem=acc_recv.at[slot, s, there, k],
            device_id=neighbour(side),
            device_id_type=MESH,
        )

    def part_copy(slot, s, side, k, there):
        return pltpu.make_async_remote_copy(
            src_ref=give.at[s, side, k],
            dst_ref=got.at[slot, s, there, k],
            send_sem=part_send.at[slot, s, side, k],
            recv_sem=part_recv.at[slot, s, there, k],
            device_id=neighbour(side),
            device_id_type=MESH,
        )

    boxes = [box_a, box_b, box_c]

    def place(st):
        return sum(bit(b) << m for m, b in enumerate(stages[st]))

    def stage_copy(o, kind, st, mask):
        return pltpu.make_async_remote_copy(
            src_ref=boxes[kind].at[o, st, place(st)],
            dst_ref=boxes[kind].at[o, st, place(st)],
            send_sem=sum_send.at[o, kind, st, mask - 1],
            recv_sem=sum_recv.at[o, kind, st, mask - 1],
            device_id=(flipped(st, mask),),
            device_id_type=MESH,
        )

    def stage_open(o, kind, st, value):
        boxes[kind][o, st, place(st)] = value
        for mask in masks(st):
            stage_copy(o, kind, st, mask).start()

    def group_open(o, kind):
        begin, count = GROUPS[kind]
        stage_open(o, kind, 0, grow[o, pl.ds(begin, count)])

    def advance(o, kind, st):
        for mask in masks(st):
            stage_copy(o, kind, st, mask).wait()
        value = boxes[kind][o, st, 0]
        for m in masks(st):
            value = value + boxes[kind][o, st, m]
        if st + 1 < len(stages):
            stage_open(o, kind, st + 1, value)
        else:
            begin, count = GROUPS[kind]
            totals[o, pl.ds(begin, count)] = value

    lap = streams * DEPTH
    agenda = {}
    taken = {}
    for o, kind, whens in [
        (0, 0, [2 * streams]),
        (0, 1, [5 * streams - 1, 5 * streams + 1]),
        (0, 2, [6 * streams - 1, 6 * streams + 1]),
        (1, 0, [lap + 2 * streams, lap + 3 * streams]),
        (1, 1, []),
        (1, 2, []),
    ]:
        for st, when in enumerate(whens[: len(stages)]):
            agenda.setdefault(when, []).append((o, kind, st))
        taken[o, kind] = min(len(whens), len(stages))

    def point(at):
        for when, steps in agenda.items():

            @pl.when(at == when)
            def _():
                for step in steps:
                    advance(*step)

    def finish(o, kind):
        for st in range(taken[o, kind], len(stages)):
            advance(o, kind, st)

    def ranks(i):
        offs = [off_ref[i, k] for k in range(slots)]
        return offs, [
            sum((offs[m] < offs[k]).astype(jnp.int32) for m in range(slots) if m != k)
            for k in range(slots)
        ]

    def sorted_slot(i, s):
        offs, rank = ranks(i)
        index, off = 0, 0
        for k in range(slots):
            index = jnp.where(rank[k] == s, k, index)
            off = jnp.where(rank[k] == s, offs[k], off)
        return index, off

    def source(i, d):
        offs, rank = ranks(i)
        index = nblk * slots
        for k in range(slots):
            index = jnp.where(offs[k] == d, i * slots + rank[k], index)
        return index

    def keep(ref, where, value):
        high, low = halves(value)
        ref[where + (pl.ds(0, width),)] = high
        ref[where + (pl.ds(width, width),)] = low

    def product(lhs, high, low):
        top = jnp.dot(lhs, high, preferred_element_type=F32)
        bottom = jnp.dot(lhs[:width], low, preferred_element_type=F32)
        return top[:width] + (top[width:] + bottom)

    def forward(s, i, begin, count):
        lhs = jnp.concatenate(
            [field[s, i + REACH + sorted_slot(i, begin + m)[1]] for m in range(count)], axis=1
        )
        span = pl.ds(pl.multiple_of(begin * tile, tile), count * tile)
        return product(lhs, fwd_high[i, span], fwd_low[i, span])

    def adjoint(s, i, begin, count):
        for m in range(count):
            k = begin + m
            parts[i * slots + k] = product(image[s, i], adj_high[i, k], adj_low[i, k])

    def edge(side, k):
        return side * (slots - REACH + k), REACH - k

    def inner(side, k):
        return (1 - side) * (REACH - k), slots - REACH + k

    middle = list(range(REACH, nblk - REACH))

    def rows_of(tl):
        return 1 + (tl + 1) // 2

    def first_row(tl):
        if isinstance(tl, int):
            return FIRST[tl]
        at = 0
        for t in range(1, SIZE):
            at = at + (FIRST[t] - FIRST[t - 1]) * jnp.int32(tl >= t)
        return at

    def repeat(count, body):
        if isinstance(count, int):
            for v in range(count):
                body(v, 0)
        else:
            lax.fori_loop(0, count, body, 0)

    def gram_rows(o, tl, s):
        base = o * SIZE

        def one(v, carry):
            if isinstance(tl, int):
                u = tl if v == 0 else 2 * v - 1 - tl % 2
            else:
                u = jnp.where(v == 0, tl, 2 * v - 1 - lax.rem(tl, 2))
            total = basis[s, base + tl, 0] * basis[s, base + u, 0]
            for i in range(1, nblk):
                total = total + basis[s, base + tl, i] * basis[s, base + u, i]
            lanes = total[:, :128]
            for c in range(128, tile, 128):
                lanes = lanes + total[:, c : c + 128]
            gacc[tl % 2, v, s] = lanes
            return carry

        repeat(rows_of(tl), one)

    def gram_close(o, tl):
        begin = first_row(tl)

        def one(v, carry):
            m = gacc[tl % 2, v].reshape(probes, 128).T
            grow[o, pl.ds(begin + v, 1), :] = jnp.sum(m, axis=0, keepdims=True)
            return carry

        repeat(rows_of(tl), one)
        for kind, last in enumerate(CLOSES):
            pl.when(tl == last)(functools.partial(group_open, o, kind))

    def gram(o, tl, s):
        gram_rows(o, tl, s)
        pl.when(s == streams - 1)(functools.partial(gram_close, o, tl))

    def phase(g, s):
        o, tl = g // DEPTH, 2 * lax.rem(g, DEPTH)
        t, slot = 2 * g, lax.rem(g, 2)
        which = ((tl == 0) & (g > 0)).astype(jnp.int32)

        @pl.when((s == 0) & (which == 1))
        def _():
            finish(0, 0)
            full = jnp.broadcast_to(provisional(totals, 0, total_rows), (128, probes)).T
            for m in range(streams):
                for c in range(0, tile, 128):
                    scale[1, m, :, pl.ds(c, 128)] = full[m * width : (m + 1) * width]

        factor = scale[which, s]
        for i in middle:
            p = acc[s, i] * factor
            basis[s, t, i] = p
            keep(field, (s, i + REACH), p)
        for side in (fast, slow):
            for k in range(REACH):
                acc_copy(slot, s, side, k, side).wait()

                @pl.when(g > 0)
                def _():
                    part_copy(slot, s, side, k, side).wait()

                i = block(side, k)
                p = (acc[s, i] + got[slot, s, side, k]) * factor
                basis[s, t, i] = p
                keep(field, (s, i + REACH), p)
                beside = (halo[slot, s, side, k] + give[s, side, k]) * factor
                keep(field, (s, beyond(side, k) + REACH), beside)
            if side is fast:
                partial = [forward(s, block(fast, k), *edge(fast, k)) for k in range(REACH)]

        def image_row(i, q):
            basis[s, t + 1, i] = q
            keep(image, (s, i), q)

        def hand_over(side):
            for k in range(REACH):
                total = None
                for r in range(REACH - k):
                    term = parts[source(block(side, r), (2 * side - 1) * (r + 1 + k))]
                    total = term if total is None else total + term
                give[s, side, k] = total
                part_copy(1 - slot, s, side, k, 1 - side).start()

        for k in range(REACH):
            i = block(slow, k)
            image_row(i, forward(s, i, 0, slots))
        for k in range(REACH):
            i = block(fast, k)
            image_row(i, partial[k] + forward(s, i, *inner(fast, k)))
        for i in middle:
            image_row(i, forward(s, i, 0, slots))

        @pl.when(g == last_pair)
        def _():
            gram(OUTER - 1, SIZE - 1, s)

        for k in range(REACH):
            adjoint(s, block(slow, k), *edge(slow, k))
        hand_over(slow)
        for k in range(REACH):
            adjoint(s, block(slow, k), *inner(slow, k))
            adjoint(s, block(fast, k), 0, slots)
        for i in middle:
            adjoint(s, i, 0, slots)
        for i in range(nblk):
            total = None
            for r in range(nblk):
                if abs(i - r) <= REACH:
                    term = parts[source(r, i - r)]
                    total = term if total is None else total + term
            acc[s, i] = total

        @pl.when(g < last_pair)
        def _():
            for k in range(REACH):
                acc_copy(1 - slot, s, slow, k, 1 - slow).start()

        hand_over(fast)

        @pl.when(g < last_pair)
        def _():
            for k in range(REACH):
                acc_copy(1 - slot, s, fast, k, 1 - fast).start()
            gram(o, tl, s)
            gram(o, tl + 1, s)

        @pl.when(g == last_pair)
        def _():
            gram(OUTER - 1, SIZE - 2, s)

        point(streams * g + s)

    grow[...] = jnp.zeros_like(grow)
    parts[nblk * slots] = jnp.zeros((width, tile), F32)
    scale[...] = jnp.ones_like(scale)
    give[...] = jnp.zeros_like(give)
    got[0] = jnp.zeros_like(got[0])
    load_start.wait()

    def turn(i):
        value = first[i].T
        for s in range(streams):
            acc[s, i] = value[s * width : (s + 1) * width]

    for k in range(REACH):
        turn(block(slow, k))
    pl.semaphore_wait(barrier, len(others))
    for s in range(streams):
        for k in range(REACH):
            acc_copy(0, s, slow, k, 1 - slow).start()
    for k in range(REACH):
        turn(block(fast, k))
    for s in range(streams):
        for k in range(REACH):
            acc_copy(0, s, fast, k, 1 - fast).start()
    for i in middle:
        turn(i)
    load_tiles.wait()
    load_offs.wait()

    def prepare(i, carry):
        for s in range(slots):
            value = raw[i, sorted_slot(i, s)[0]]
            high, low = halves(value)
            adj_high[i, s] = high
            adj_low[i, s] = low
            high, low = halves(value.T)
            fwd_high[i, pl.ds(s * tile, tile)] = high
            fwd_low[i, pl.ds(s * tile, tile)] = low
        return carry

    lax.fori_loop(0, nblk, prepare, 0)

    def pair(g, carry):
        def stream(s, c):
            phase(g, s)
            return c

        return lax.fori_loop(0, streams, stream, carry)

    lax.fori_loop(0, last_pair + 1, pair, 0)

    def last(s):
        slot = (last_pair + 1) % 2
        for side in (fast, slow):
            for k in range(REACH):
                i = block(side, k)
                part_copy(slot, s, side, k, side).wait()
                ends[s, i] = acc[s, i] + got[slot, s, side, k]
        for i in middle:
            ends[s, i] = acc[s, i]

    for s in range(streams - 1):
        last(s)
    advance(OUTER - 1, 2, 0)
    advance(OUTER - 1, 1, 0)
    last(streams - 1)
    for kind in (2, 1, 0):
        taken[OUTER - 1, kind] = max(taken[OUTER - 1, kind], 1)
        finish(OUTER - 1, kind)
    if OUTER > 1:
        for kind in range(1, len(GROUPS)):
            finish(0, kind)


def closing(total_rows, totals, ends, gram_ref, final_ref):
    streams, nblk, _, _ = ends.shape
    true = jnp.ones((1, totals.shape[2]), F32)
    for o in range(OUTER):
        for a in range(SIZE):
            for b in range(SIZE):
                x, y = a % DEPTH, b % DEPTH
                if a // DEPTH == b // DEPTH:
                    row = FIRST[x + y + a // DEPTH]
                else:
                    x, y = (x, y) if a < DEPTH else (y, x)
                    row = FIRST[2 * y + 1] + 1 + x if x <= y else FIRST[2 * x] + 1 + y
                value = totals[o, row : row + 1, :] / total_rows
                gram_ref[o, pl.ds(a * SIZE + b, 1), :] = value * true * true
        row = FIRST[SIZE - 1]
        corner = totals[o, row : row + 1, :] / total_rows * true * true
        norm = true / jnp.sqrt(corner + 0.25)
        if o < OUTER - 1:
            true = norm / provisional(totals, o, total_rows)
    for i in range(nblk):
        value = jnp.concatenate([ends[s, i] for s in range(streams)], axis=0)
        final_ref[i] = value.T * norm


def on_device(tiles, offsets, start):
    n = lax.axis_size("blk")
    levels = n.bit_length() - 1
    assert n == 1 << levels
    bits = [[0, 3, 4], [1, 2]] + [[b, b + 1] for b in range(5, levels, 2)]
    stages = [kept for group in bits if (kept := [b for b in group if b < levels])]
    nblk, slots, tile, _ = tiles.shape
    rows, probes = start.shape
    assert nblk >= 2 * REACH and slots >= REACH and OUTER == 2
    streams = STREAMS
    width = probes // streams
    dma = pltpu.SemaphoreType.DMA
    wide = (nblk, slots * tile, tile)
    square = (nblk, slots, tile, tile)
    whole = pl.BlockSpec(memory_space=pltpu.VMEM)
    operands = (offsets, tiles, start.reshape(nblk, tile, probes))
    totals, ends = pl.pallas_call(
        functools.partial(kernel, n, stages, float(rows * n)),
        out_shape=(
            pltpu.VMEM((OUTER, 32, probes), F32),
            pltpu.VMEM((streams, nblk, width, tile), F32),
        ),
        in_specs=[
            pl.BlockSpec(memory_space=pl.ANY),
            pl.BlockSpec(memory_space=pl.ANY),
            pl.BlockSpec(memory_space=pl.ANY),
        ],
        out_specs=(whole, whole),
        scratch_shapes=[
            pltpu.SMEM(offsets.shape, jnp.int32),
            pltpu.VMEM(tiles.shape, F32),
            pltpu.VMEM((nblk, tile, probes), F32),
            pltpu.VMEM(wide, BF16),
            pltpu.VMEM(wide, BF16),
            pltpu.VMEM(square, BF16),
            pltpu.VMEM(square, BF16),
            pltpu.VMEM((streams, OUTER * SIZE, nblk, width, tile), F32),
            pltpu.VMEM((streams, nblk + 2 * REACH, 2 * width, tile), BF16),
            pltpu.VMEM((streams, nblk, 2 * width, tile), BF16),
            pltpu.VMEM((nblk * slots + 1, width, tile), F32),
            pltpu.VMEM((streams, nblk, width, tile), F32),
            pltpu.VMEM((2, streams, 2, REACH, width, tile), F32),
            pltpu.VMEM((streams, 2, REACH, width, tile), F32),
            pltpu.VMEM((2, streams, 2, REACH, width, tile), F32),
            pltpu.VMEM((2, streams, width, tile), F32),
            pltpu.VMEM((2, 1 + DEPTH, streams, width, 128), F32),
            pltpu.VMEM((OUTER, 32, probes), F32),
        ]
        + [pltpu.VMEM((OUTER, len(stages), 8, count, probes), F32) for _, count in GROUPS]
        + [
            dma((3,)),
            dma((2, streams, 2, REACH)),
            dma((2, streams, 2, REACH)),
            dma((2, streams, 2, REACH)),
            dma((2, streams, 2, REACH)),
            dma((OUTER, len(GROUPS), len(stages), 7)),
            dma((OUTER, len(GROUPS), len(stages), 7)),
        ],
        compiler_params=pltpu.CompilerParams(
            collective_id=0, has_side_effects=True, vmem_limit_bytes=48 << 20
        ),
    )(*[pltpu.with_memory_space_constraint(x, pltpu.HBM) for x in operands])
    grams, final = pl.pallas_call(
        functools.partial(closing, float(rows * n)),
        out_shape=(
            jax.ShapeDtypeStruct((OUTER, SIZE * SIZE, probes), F32),
            jax.ShapeDtypeStruct((nblk, tile, probes), F32),
        ),
        in_specs=[whole, whole],
        out_specs=(whole, whole),
        compiler_params=pltpu.CompilerParams(vmem_limit_bytes=8 << 20),
    )(totals, ends)
    return grams.reshape(OUTER, SIZE, SIZE, probes), final.reshape(rows, probes)


def solution(mesh):
    placed = (P("blk", None, None, None), P("blk", None), P("blk", None))
    return jax.shard_map(
        on_device, mesh=mesh, in_specs=placed, out_specs=(P(), P("blk", None)), check_vma=False
    )
```

```python
import functools

import jax
import jax.numpy as jnp
from jax import lax
from jax.experimental import pallas as pl
from jax.experimental.pallas import tpu as pltpu
from jax.sharding import PartitionSpec as P

REACH = 2
OUTER = 2
DEPTH = 4
SIZE = 2 * DEPTH
STREAMS = 2
FIRST = [0, 1, 3, 5, 8, 11, 15, 24]
GROUPS = [(0, 8), (8, 16), (24, 8)]
CLOSES = [3, 6, 7]
GAUGE = 3
GROWTH = 2.0 ** (14 * (SIZE - 1 - GAUGE))
MESH = pl.DeviceIdType.MESH
F32 = jnp.float32
BF16 = jnp.bfloat16


def halves(x):
    high = x.astype(BF16)
    return high, (x - high.astype(F32)).astype(BF16)


def provisional(totals, o, total_rows):
    row = FIRST[GAUGE]
    return 1.0 / jnp.sqrt(totals[o, row : row + 1, :] / total_rows * GROWTH + 0.25)


def kernel(
    n,
    stages,
    total_rows,
    off_hbm,
    tiles_hbm,
    start_hbm,
    totals,
    ends,
    off_ref,
    raw,
    first,
    fwd_high,
    fwd_low,
    adj_high,
    adj_low,
    basis,
    field,
    image,
    parts,
    acc,
    halo,
    give,
    got,
    scale,
    gacc,
    grow,
    box_a,
    box_b,
    box_c,
    start_sem,
    load_sem,
    acc_send,
    acc_recv,
    part_send,
    part_recv,
    sum_send,
    sum_recv,
):
    nblk, slots, tile, _ = raw.shape
    streams = basis.shape[0]
    width = basis.shape[3]
    probes = streams * width
    last_pair = OUTER * DEPTH - 1
    me = lax.axis_index("blk")
    slow = lax.rem(me, 2)
    fast = 1 - slow

    def load_start(i):
        return pltpu.make_async_copy(start_hbm.at[i], first.at[i], start_sem.at[i])

    load_tiles = pltpu.make_async_copy(tiles_hbm, raw, load_sem.at[0])
    load_offs = pltpu.make_async_copy(off_hbm, off_ref, load_sem.at[1])

    def block(side, k):
        return side * (nblk - 1) + k * (1 - 2 * side)

    def beyond(side, k):
        return side * (nblk + 1 + 2 * k) - 1 - k

    for side in (slow, fast):
        for k in range(REACH):
            load_start(block(side, k)).start()
    for i in range(REACH, nblk - REACH):
        load_start(i).start()
    load_tiles.start()
    load_offs.start()

    barrier = pltpu.get_barrier_semaphore()

    def bit(b):
        return lax.rem(me // (1 << b), 2)

    def flipped(st, mask):
        other = me
        for m, b in enumerate(stages[st]):
            if mask >> m & 1:
                other = other + (1 << b) * (1 - 2 * bit(b))
        return other

    def masks(st):
        return range(1, 1 << len(stages[st]))

    others = [lax.rem(me + n - 1, n), lax.rem(me + 1, n)]
    others += [flipped(st, mask) for st in range(len(stages)) for mask in masks(st)]
    for other in others:
        pl.semaphore_signal(barrier, inc=1, device_id=(other,), device_id_type=MESH)

    def neighbour(side):
        return (lax.rem(me + n - 1 + 2 * side, n),)

    def acc_copy(slot, s, side, k, there):
        return pltpu.make_async_remote_copy(
            src_ref=acc.at[s, block(side, k)],
            dst_ref=halo.at[slot, s, there, k],
            send_sem=acc_send.at[slot, s, side, k],
            recv_sem=acc_recv.at[slot, s, there, k],
            device_id=neighbour(side),
            device_id_type=MESH,
        )

    def part_copy(slot, s, side, k, there):
        return pltpu.make_async_remote_copy(
            src_ref=give.at[s, side, k],
            dst_ref=got.at[slot, s, there, k],
            send_sem=part_send.at[slot, s, side, k],
            recv_sem=part_recv.at[slot, s, there, k],
            device_id=neighbour(side),
            device_id_type=MESH,
        )

    boxes = [box_a, box_b, box_c]

    def place(st):
        return sum(bit(b) << m for m, b in enumerate(stages[st]))

    def stage_copy(o, kind, st, mask):
        return pltpu.make_async_remote_copy(
            src_ref=boxes[kind].at[o, st, place(st)],
            dst_ref=boxes[kind].at[o, st, place(st)],
            send_sem=sum_send.at[o, kind, st, mask - 1],
            recv_sem=sum_recv.at[o, kind, st, mask - 1],
            device_id=(flipped(st, mask),),
            device_id_type=MESH,
        )

    def stage_open(o, kind, st, value):
        boxes[kind][o, st, place(st)] = value
        for mask in masks(st):
            stage_copy(o, kind, st, mask).start()

    def group_open(o, kind):
        begin, count = GROUPS[kind]
        stage_open(o, kind, 0, grow[o, pl.ds(begin, count)])

    def advance(o, kind, st):
        for mask in masks(st):
            stage_copy(o, kind, st, mask).wait()
        value = boxes[kind][o, st, 0]
        for m in masks(st):
            value = value + boxes[kind][o, st, m]
        if st + 1 < len(stages):
            stage_open(o, kind, st + 1, value)
        else:
            begin, count = GROUPS[kind]
            totals[o, pl.ds(begin, count)] = value

    lap = streams * DEPTH
    agenda = {}
    taken = {}
    for o, kind, whens in [
        (0, 0, [2 * streams]),
        (0, 1, [5 * streams - 1, 5 * streams + 1]),
        (0, 2, [6 * streams - 1, 6 * streams + 1]),
        (1, 0, [lap + 2 * streams, lap + 3 * streams]),
        (1, 1, []),
        (1, 2, []),
    ]:
        for st, when in enumerate(whens[: len(stages)]):
            agenda.setdefault(when, []).append((o, kind, st))
        taken[o, kind] = min(len(whens), len(stages))

    def point(at):
        for when, steps in agenda.items():

            @pl.when(at == when)
            def _():
                for step in steps:
                    advance(*step)

    def finish(o, kind):
        for st in range(taken[o, kind], len(stages)):
            advance(o, kind, st)

    def ranks(i):
        offs = [off_ref[i, k] for k in range(slots)]
        return offs, [
            sum((offs[m] < offs[k]).astype(jnp.int32) for m in range(slots) if m != k)
            for k in range(slots)
        ]

    def sorted_slot(i, s):
        offs, rank = ranks(i)
        index, off = 0, 0
        for k in range(slots):
            index = jnp.where(rank[k] == s, k, index)
            off = jnp.where(rank[k] == s, offs[k], off)
        return index, off

    def source(i, d):
        offs, rank = ranks(i)
        index = nblk * slots
        for k in range(slots):
            index = jnp.where(offs[k] == d, i * slots + rank[k], index)
        return index

    def keep(ref, where, value):
        high, low = halves(value)
        ref[where + (pl.ds(0, width),)] = high
        ref[where + (pl.ds(width, width),)] = low

    def product(lhs, high, low):
        top = jnp.dot(lhs, high, preferred_element_type=F32)
        bottom = jnp.dot(lhs[:width], low, preferred_element_type=F32)
        return top[:width] + (top[width:] + bottom)

    def forward(s, i, begin, count):
        lhs = jnp.concatenate(
            [field[s, i + REACH + sorted_slot(i, begin + m)[1]] for m in range(count)], axis=1
        )
        span = pl.ds(pl.multiple_of(begin * tile, tile), count * tile)
        return product(lhs, fwd_high[i, span], fwd_low[i, span])

    def adjoint(s, i, begin, count):
        for m in range(count):
            k = begin + m
            parts[i * slots + k] = product(image[s, i], adj_high[i, k], adj_low[i, k])

    def edge(side, k):
        return side * (slots - REACH + k), REACH - k

    def inner(side, k):
        return (1 - side) * (REACH - k), slots - REACH + k

    middle = list(range(REACH, nblk - REACH))

    def rows_of(tl):
        return 1 + (tl + 1) // 2

    def first_row(tl):
        if isinstance(tl, int):
            return FIRST[tl]
        at = 0
        for t in range(1, SIZE):
            at = at + (FIRST[t] - FIRST[t - 1]) * jnp.int32(tl >= t)
        return at

    def repeat(count, body):
        if isinstance(count, int):
            for v in range(count):
                body(v, 0)
        else:
            lax.fori_loop(0, count, body, 0)

    def gram_rows(o, tl, s):
        base = o * SIZE

        def one(v, carry):
            if isinstance(tl, int):
                u = tl if v == 0 else 2 * v - 1 - tl % 2
            else:
                u = jnp.where(v == 0, tl, 2 * v - 1 - lax.rem(tl, 2))
            total = basis[s, base + tl, 0] * basis[s, base + u, 0]
            for i in range(1, nblk):
                total = total + basis[s, base + tl, i] * basis[s, base + u, i]
            lanes = total[:, :128]
            for c in range(128, tile, 128):
                lanes = lanes + total[:, c : c + 128]
            gacc[tl % 2, v, s] = lanes
            return carry

        repeat(rows_of(tl), one)

    def gram_close(o, tl):
        begin = first_row(tl)

        def one(v, carry):
            m = gacc[tl % 2, v].reshape(probes, 128).T
            grow[o, pl.ds(begin + v, 1), :] = jnp.sum(m, axis=0, keepdims=True)
            return carry

        repeat(rows_of(tl), one)
        for kind, last in enumerate(CLOSES):
            pl.when(tl == last)(functools.partial(group_open, o, kind))

    def gram(o, tl, s):
        gram_rows(o, tl, s)
        pl.when(s == streams - 1)(functools.partial(gram_close, o, tl))

    def phase(g, s):
        o, tl = g // DEPTH, 2 * lax.rem(g, DEPTH)
        t, slot = 2 * g, lax.rem(g, 2)
        which = ((tl == 0) & (g > 0)).astype(jnp.int32)

        @pl.when((s == 0) & (which == 1))
        def _():
            finish(0, 0)
            full = jnp.broadcast_to(provisional(totals, 0, total_rows), (128, probes)).T
            for m in range(streams):
                for c in range(0, tile, 128):
                    scale[1, m, :, pl.ds(c, 128)] = full[m * width : (m + 1) * width]

        factor = scale[which, s]
        for i in middle:
            p = acc[s, i] * factor
            basis[s, t, i] = p
            keep(field, (s, i + REACH), p)
        for side in (fast, slow):
            for k in range(REACH):
                acc_copy(slot, s, side, k, side).wait()

                @pl.when(g > 0)
                def _():
                    part_copy(slot, s, side, k, side).wait()

                i = block(side, k)
                p = (acc[s, i] + got[slot, s, side, k]) * factor
                basis[s, t, i] = p
                keep(field, (s, i + REACH), p)
                beside = (halo[slot, s, side, k] + give[s, side, k]) * factor
                keep(field, (s, beyond(side, k) + REACH), beside)
            if side is fast:
                partial = [forward(s, block(fast, k), *edge(fast, k)) for k in range(REACH)]

        @pl.when(g == last_pair)
        def _():
            gram(OUTER - 1, SIZE - 2, s)

        def image_row(i, q):
            basis[s, t + 1, i] = q
            keep(image, (s, i), q)

        def hand_over(side):
            for k in range(REACH):
                total = None
                for r in range(REACH - k):
                    term = parts[source(block(side, r), (2 * side - 1) * (r + 1 + k))]
                    total = term if total is None else total + term
                give[s, side, k] = total
                part_copy(1 - slot, s, side, k, 1 - side).start()

        for k in range(REACH):
            i = block(slow, k)
            image_row(i, forward(s, i, 0, slots))
        for k in range(REACH):
            i = block(fast, k)
            image_row(i, partial[k] + forward(s, i, *inner(fast, k)))
        for i in middle:
            image_row(i, forward(s, i, 0, slots))

        @pl.when(g == last_pair)
        def _():
            gram(OUTER - 1, SIZE - 1, s)

        for k in range(REACH):
            adjoint(s, block(slow, k), *edge(slow, k))
        hand_over(slow)
        for k in range(REACH):
            adjoint(s, block(slow, k), *inner(slow, k))
            adjoint(s, block(fast, k), 0, slots)
        for i in middle:
            adjoint(s, i, 0, slots)
        for i in range(nblk):
            total = None
            for r in range(nblk):
                if abs(i - r) <= REACH:
                    term = parts[source(r, i - r)]
                    total = term if total is None else total + term
            acc[s, i] = total

        @pl.when(g < last_pair)
        def _():
            for k in range(REACH):
                acc_copy(1 - slot, s, slow, k, 1 - slow).start()

        hand_over(fast)

        @pl.when(g < last_pair)
        def _():
            for k in range(REACH):
                acc_copy(1 - slot, s, fast, k, 1 - fast).start()
            gram(o, tl, s)
            gram(o, tl + 1, s)

        point(streams * g + s)

    grow[...] = jnp.zeros_like(grow)
    parts[nblk * slots] = jnp.zeros((width, tile), F32)
    scale[...] = jnp.ones_like(scale)
    give[...] = jnp.zeros_like(give)
    got[0] = jnp.zeros_like(got[0])

    def turn(i):
        load_start(i).wait()
        value = first[i].T
        for s in range(streams):
            acc[s, i] = value[s * width : (s + 1) * width]

    for k in range(REACH):
        turn(block(slow, k))
    pl.semaphore_wait(barrier, len(others))
    for s in range(streams):
        for k in range(REACH):
            acc_copy(0, s, slow, k, 1 - slow).start()
    for k in range(REACH):
        turn(block(fast, k))
    for s in range(streams):
        for k in range(REACH):
            acc_copy(0, s, fast, k, 1 - fast).start()
    for i in middle:
        turn(i)
    load_tiles.wait()
    load_offs.wait()

    def prepare(i, carry):
        for s in range(slots):
            value = raw[i, sorted_slot(i, s)[0]]
            high, low = halves(value)
            adj_high[i, s] = high
            adj_low[i, s] = low
            high, low = halves(value.T)
            fwd_high[i, pl.ds(s * tile, tile)] = high
            fwd_low[i, pl.ds(s * tile, tile)] = low
        return carry

    lax.fori_loop(0, nblk, prepare, 0)

    def pair(g, carry):
        def stream(s, c):
            phase(g, s)
            return c

        return lax.fori_loop(0, streams, stream, carry)

    lax.fori_loop(0, last_pair + 1, pair, 0)

    def last(s):
        slot = (last_pair + 1) % 2
        for side in (fast, slow):
            for k in range(REACH):
                i = block(side, k)
                part_copy(slot, s, side, k, side).wait()
                ends[s, i] = acc[s, i] + got[slot, s, side, k]
        for i in middle:
            ends[s, i] = acc[s, i]

    for s in range(streams - 1):
        last(s)
    advance(OUTER - 1, 1, 0)
    advance(OUTER - 1, 2, 0)
    last(streams - 1)
    for kind in (1, 2, 0):
        taken[OUTER - 1, kind] = max(taken[OUTER - 1, kind], 1)
        finish(OUTER - 1, kind)
    if OUTER > 1:
        for kind in range(1, len(GROUPS)):
            finish(0, kind)


def closing(total_rows, totals, ends, gram_ref, final_ref):
    streams, nblk, _, _ = ends.shape
    true = jnp.ones((1, totals.shape[2]), F32)
    for o in range(OUTER):
        for a in range(SIZE):
            for b in range(SIZE):
                x, y = a % DEPTH, b % DEPTH
                if a // DEPTH == b // DEPTH:
                    row = FIRST[x + y + a // DEPTH]
                else:
                    x, y = (x, y) if a < DEPTH else (y, x)
                    row = FIRST[2 * y + 1] + 1 + x if x <= y else FIRST[2 * x] + 1 + y
                value = totals[o, row : row + 1, :] / total_rows
                gram_ref[o, pl.ds(a * SIZE + b, 1), :] = value * true * true
        row = FIRST[SIZE - 1]
        corner = totals[o, row : row + 1, :] / total_rows * true * true
        norm = true / jnp.sqrt(corner + 0.25)
        if o < OUTER - 1:
            true = norm / provisional(totals, o, total_rows)
    for i in range(nblk):
        value = jnp.concatenate([ends[s, i] for s in range(streams)], axis=0)
        final_ref[i] = value.T * norm


def on_device(tiles, offsets, start):
    n = lax.axis_size("blk")
    levels = n.bit_length() - 1
    assert n == 1 << levels
    bits = [[0, 3, 4], [1, 2]] + [[b, b + 1] for b in range(5, levels, 2)]
    stages = [kept for group in bits if (kept := [b for b in group if b < levels])]
    nblk, slots, tile, _ = tiles.shape
    rows, probes = start.shape
    assert nblk >= 2 * REACH and slots >= REACH and OUTER == 2
    streams = STREAMS
    width = probes // streams
    dma = pltpu.SemaphoreType.DMA
    wide = (nblk, slots * tile, tile)
    square = (nblk, slots, tile, tile)
    whole = pl.BlockSpec(memory_space=pltpu.VMEM)
    operands = (offsets, tiles, start.reshape(nblk, tile, probes))
    totals, ends = pl.pallas_call(
        functools.partial(kernel, n, stages, float(rows * n)),
        out_shape=(
            pltpu.VMEM((OUTER, 32, probes), F32),
            pltpu.VMEM((streams, nblk, width, tile), F32),
        ),
        in_specs=[
            pl.BlockSpec(memory_space=pl.ANY),
            pl.BlockSpec(memory_space=pl.ANY),
            pl.BlockSpec(memory_space=pl.ANY),
        ],
        out_specs=(whole, whole),
        scratch_shapes=[
            pltpu.SMEM(offsets.shape, jnp.int32),
            pltpu.VMEM(tiles.shape, F32),
            pltpu.VMEM((nblk, tile, probes), F32),
            pltpu.VMEM(wide, BF16),
            pltpu.VMEM(wide, BF16),
            pltpu.VMEM(square, BF16),
            pltpu.VMEM(square, BF16),
            pltpu.VMEM((streams, OUTER * SIZE, nblk, width, tile), F32),
            pltpu.VMEM((streams, nblk + 2 * REACH, 2 * width, tile), BF16),
            pltpu.VMEM((streams, nblk, 2 * width, tile), BF16),
            pltpu.VMEM((nblk * slots + 1, width, tile), F32),
            pltpu.VMEM((streams, nblk, width, tile), F32),
            pltpu.VMEM((2, streams, 2, REACH, width, tile), F32),
            pltpu.VMEM((streams, 2, REACH, width, tile), F32),
            pltpu.VMEM((2, streams, 2, REACH, width, tile), F32),
            pltpu.VMEM((2, streams, width, tile), F32),
            pltpu.VMEM((2, 1 + DEPTH, streams, width, 128), F32),
            pltpu.VMEM((OUTER, 32, probes), F32),
        ]
        + [pltpu.VMEM((OUTER, len(stages), 8, count, probes), F32) for _, count in GROUPS]
        + [
            dma((nblk,)),
            dma((2,)),
            dma((2, streams, 2, REACH)),
            dma((2, streams, 2, REACH)),
            dma((2, streams, 2, REACH)),
            dma((2, streams, 2, REACH)),
            dma((OUTER, len(GROUPS), len(stages), 7)),
            dma((OUTER, len(GROUPS), len(stages), 7)),
        ],
        compiler_params=pltpu.CompilerParams(
            collective_id=0, has_side_effects=True, vmem_limit_bytes=48 << 20
        ),
    )(*[pltpu.with_memory_space_constraint(x, pltpu.HBM) for x in operands])
    grams, final = pl.pallas_call(
        functools.partial(closing, float(rows * n)),
        out_shape=(
            jax.ShapeDtypeStruct((OUTER, SIZE * SIZE, probes), F32),
            jax.ShapeDtypeStruct((nblk, tile, probes), F32),
        ),
        in_specs=[whole, whole],
        out_specs=(whole, whole),
        compiler_params=pltpu.CompilerParams(vmem_limit_bytes=8 << 20),
    )(totals, ends)
    return grams.reshape(OUTER, SIZE, SIZE, probes), final.reshape(rows, probes)


def solution(mesh):
    placed = (P("blk", None, None, None), P("blk", None), P("blk", None))
    return jax.shard_map(
        on_device, mesh=mesh, in_specs=placed, out_specs=(P(), P("blk", None)), check_vma=False
    )
```

```python
import functools

import jax
import jax.numpy as jnp
from jax import lax
from jax.experimental import pallas as pl
from jax.experimental.pallas import tpu as pltpu
from jax.sharding import PartitionSpec as P

REACH = 2
OUTER = 2
DEPTH = 4
SIZE = 2 * DEPTH
STREAMS = 2
FIRST = [0, 1, 3, 5, 8, 11, 16, 24]
GROUPS = [(0, 8), (8, 8), (16, 8), (24, 8)]
CLOSES = [3, 5, 6, 7]
GAUGE = 3
GROWTH = 2.0 ** (14 * (SIZE - 1 - GAUGE))
MESH = pl.DeviceIdType.MESH
F32 = jnp.float32
BF16 = jnp.bfloat16


def halves(x):
    high = x.astype(BF16)
    return high, (x - high.astype(F32)).astype(BF16)


def provisional(totals, o, total_rows):
    row = FIRST[GAUGE]
    return 1.0 / jnp.sqrt(totals[o, row : row + 1, :] / total_rows * GROWTH + 0.25)


def kernel(
    n,
    stages,
    total_rows,
    off_hbm,
    tiles_hbm,
    start_hbm,
    totals,
    ends,
    off_ref,
    raw,
    first,
    fwd_high,
    fwd_low,
    adj_high,
    adj_low,
    basis,
    field,
    image,
    parts,
    acc,
    halo,
    give,
    got,
    scale,
    gacc,
    grow,
    box_a,
    box_b,
    box_c,
    box_d,
    start_sem,
    load_sem,
    acc_send,
    acc_recv,
    part_send,
    part_recv,
    sum_send,
    sum_recv,
):
    nblk, slots, tile, _ = raw.shape
    streams = basis.shape[0]
    width = basis.shape[3]
    probes = streams * width
    last_pair = OUTER * DEPTH - 1
    me = lax.axis_index("blk")
    slow = lax.rem(me, 2)
    fast = 1 - slow

    def load_start(i):
        return pltpu.make_async_copy(start_hbm.at[i], first.at[i], start_sem.at[i])

    load_tiles = pltpu.make_async_copy(tiles_hbm, raw, load_sem.at[0])
    load_offs = pltpu.make_async_copy(off_hbm, off_ref, load_sem.at[1])

    def block(side, k):
        return side * (nblk - 1) + k * (1 - 2 * side)

    def beyond(side, k):
        return side * (nblk + 1 + 2 * k) - 1 - k

    for side in (slow, fast):
        for k in range(REACH):
            load_start(block(side, k)).start()
    for i in range(REACH, nblk - REACH):
        load_start(i).start()
    load_tiles.start()
    load_offs.start()

    barrier = pltpu.get_barrier_semaphore()

    def bit(b):
        return lax.rem(me // (1 << b), 2)

    def flipped(st, mask):
        other = me
        for m, b in enumerate(stages[st]):
            if mask >> m & 1:
                other = other + (1 << b) * (1 - 2 * bit(b))
        return other

    def masks(st):
        return range(1, 1 << len(stages[st]))

    others = [lax.rem(me + n - 1, n), lax.rem(me + 1, n)]
    others += [flipped(st, mask) for st in range(len(stages)) for mask in masks(st)]
    for other in others:
        pl.semaphore_signal(barrier, inc=1, device_id=(other,), device_id_type=MESH)

    def neighbour(side):
        return (lax.rem(me + n - 1 + 2 * side, n),)

    def acc_copy(slot, s, side, k, there):
        return pltpu.make_async_remote_copy(
            src_ref=acc.at[s, block(side, k)],
            dst_ref=halo.at[slot, s, there, k],
            send_sem=acc_send.at[slot, s, side, k],
            recv_sem=acc_recv.at[slot, s, there, k],
            device_id=neighbour(side),
            device_id_type=MESH,
        )

    def part_copy(slot, s, side, k, there):
        return pltpu.make_async_remote_copy(
            src_ref=give.at[s, side, k],
            dst_ref=got.at[slot, s, there, k],
            send_sem=part_send.at[slot, s, side, k],
            recv_sem=part_recv.at[slot, s, there, k],
            device_id=neighbour(side),
            device_id_type=MESH,
        )

    boxes = [box_a, box_b, box_c, box_d]

    def place(st):
        return sum(bit(b) << m for m, b in enumerate(stages[st]))

    def stage_copy(o, kind, st, mask):
        return pltpu.make_async_remote_copy(
            src_ref=boxes[kind].at[o, st, place(st)],
            dst_ref=boxes[kind].at[o, st, place(st)],
            send_sem=sum_send.at[o, kind, st, mask - 1],
            recv_sem=sum_recv.at[o, kind, st, mask - 1],
            device_id=(flipped(st, mask),),
            device_id_type=MESH,
        )

    def stage_open(o, kind, st, value):
        boxes[kind][o, st, place(st)] = value
        for mask in masks(st):
            stage_copy(o, kind, st, mask).start()

    def group_open(o, kind):
        begin, count = GROUPS[kind]
        stage_open(o, kind, 0, grow[o, pl.ds(begin, count)])

    def advance(o, kind, st):
        for mask in masks(st):
            stage_copy(o, kind, st, mask).wait()
        value = boxes[kind][o, st, 0]
        for m in masks(st):
            value = value + boxes[kind][o, st, m]
        if st + 1 < len(stages):
            stage_open(o, kind, st + 1, value)
        else:
            begin, count = GROUPS[kind]
            totals[o, pl.ds(begin, count)] = value

    lap = streams * DEPTH
    agenda = {}
    taken = {}
    for o, kind, whens in [
        (0, 0, [2 * streams]),
        (0, 1, [4 * streams - 1, 5 * streams - 1]),
        (0, 2, [5 * streams, 6 * streams]),
        (0, 3, [6 * streams - 1, 7 * streams - 1]),
        (1, 0, [lap + 2 * streams, lap + 3 * streams]),
        (1, 1, [lap + 3 * streams, lap + 4 * streams - 1]),
        (1, 2, []),
        (1, 3, []),
    ]:
        for st, when in enumerate(whens[: len(stages)]):
            agenda.setdefault(when, []).append((o, kind, st))
        taken[o, kind] = min(len(whens), len(stages))

    def point(at):
        for when, steps in agenda.items():

            @pl.when(at == when)
            def _():
                for step in steps:
                    advance(*step)

    def finish(o, kind):
        for st in range(taken[o, kind], len(stages)):
            advance(o, kind, st)

    def ranks(i):
        offs = [off_ref[i, k] for k in range(slots)]
        return offs, [
            sum((offs[m] < offs[k]).astype(jnp.int32) for m in range(slots) if m != k)
            for k in range(slots)
        ]

    def sorted_slot(i, s):
        offs, rank = ranks(i)
        index, off = 0, 0
        for k in range(slots):
            index = jnp.where(rank[k] == s, k, index)
            off = jnp.where(rank[k] == s, offs[k], off)
        return index, off

    def source(i, d):
        offs, rank = ranks(i)
        index = nblk * slots
        for k in range(slots):
            index = jnp.where(offs[k] == d, i * slots + rank[k], index)
        return index

    def keep(ref, where, value):
        high, low = halves(value)
        ref[where + (pl.ds(0, width),)] = high
        ref[where + (pl.ds(width, width),)] = low

    def product(lhs, high, low):
        top = jnp.dot(lhs, high, preferred_element_type=F32)
        bottom = jnp.dot(lhs[:width], low, preferred_element_type=F32)
        return top[:width] + (top[width:] + bottom)

    def forward(s, i, begin, count):
        lhs = jnp.concatenate(
            [field[s, i + REACH + sorted_slot(i, begin + m)[1]] for m in range(count)], axis=1
        )
        span = pl.ds(pl.multiple_of(begin * tile, tile), count * tile)
        return product(lhs, fwd_high[i, span], fwd_low[i, span])

    def adjoint(s, i, begin, count):
        for m in range(count):
            k = begin + m
            parts[i * slots + k] = product(image[s, i], adj_high[i, k], adj_low[i, k])

    def edge(side, k):
        return side * (slots - REACH + k), REACH - k

    def inner(side, k):
        return (1 - side) * (REACH - k), slots - REACH + k

    middle = list(range(REACH, nblk - REACH))

    def rows_of(tl):
        return 1 + (tl + 1) // 2

    def first_row(tl):
        if isinstance(tl, int):
            return FIRST[tl]
        at = 0
        for t in range(1, SIZE):
            at = at + (FIRST[t] - FIRST[t - 1]) * jnp.int32(tl >= t)
        return at

    def repeat(count, body):
        if isinstance(count, int):
            for v in range(count):
                body(v, 0)
        else:
            lax.fori_loop(0, count, body, 0)

    def gram_rows(o, tl, s):
        base = o * SIZE

        def one(v, carry):
            if isinstance(tl, int):
                u = tl if v == 0 else 2 * v - 1 - tl % 2
            else:
                u = jnp.where(v == 0, tl, 2 * v - 1 - lax.rem(tl, 2))
            total = basis[s, base + tl, 0] * basis[s, base + u, 0]
            for i in range(1, nblk):
                total = total + basis[s, base + tl, i] * basis[s, base + u, i]
            lanes = total[:, :128]
            for c in range(128, tile, 128):
                lanes = lanes + total[:, c : c + 128]
            gacc[tl % 2, v, s] = lanes
            return carry

        repeat(rows_of(tl), one)

    def gram_close(o, tl):
        begin = first_row(tl)

        def one(v, carry):
            m = gacc[tl % 2, v].reshape(probes, 128).T
            grow[o, pl.ds(begin + v, 1), :] = jnp.sum(m, axis=0, keepdims=True)
            return carry

        repeat(rows_of(tl), one)
        for kind, last in enumerate(CLOSES):
            pl.when(tl == last)(functools.partial(group_open, o, kind))

    def gram(o, tl, s):
        gram_rows(o, tl, s)
        pl.when(s == streams - 1)(functools.partial(gram_close, o, tl))

    def phase(g, s):
        o, tl = g // DEPTH, 2 * lax.rem(g, DEPTH)
        t, slot = 2 * g, lax.rem(g, 2)
        which = ((tl == 0) & (g > 0)).astype(jnp.int32)

        @pl.when((s == 0) & (which == 1))
        def _():
            finish(0, 0)
            full = jnp.broadcast_to(provisional(totals, 0, total_rows), (128, probes)).T
            for m in range(streams):
                for c in range(0, tile, 128):
                    scale[1, m, :, pl.ds(c, 128)] = full[m * width : (m + 1) * width]

        factor = scale[which, s]
        for i in middle:
            p = acc[s, i] * factor
            basis[s, t, i] = p
            keep(field, (s, i + REACH), p)
        for side in (fast, slow):
            for k in range(REACH):
                acc_copy(slot, s, side, k, side).wait()

                @pl.when(g > 0)
                def _():
                    part_copy(slot, s, side, k, side).wait()

                i = block(side, k)
                p = (acc[s, i] + got[slot, s, side, k]) * factor
                basis[s, t, i] = p
                keep(field, (s, i + REACH), p)
                beside = (halo[slot, s, side, k] + give[s, side, k]) * factor
                keep(field, (s, beyond(side, k) + REACH), beside)
            if side is fast:
                partial = [forward(s, block(fast, k), *edge(fast, k)) for k in range(REACH)]

        @pl.when(g == last_pair)
        def _():
            gram(OUTER - 1, SIZE - 2, s)

        def image_row(i, q):
            basis[s, t + 1, i] = q
            keep(image, (s, i), q)

        def hand_over(side):
            for k in range(REACH):
                total = None
                for r in range(REACH - k):
                    term = parts[source(block(side, r), (2 * side - 1) * (r + 1 + k))]
                    total = term if total is None else total + term
                give[s, side, k] = total
                part_copy(1 - slot, s, side, k, 1 - side).start()

        for k in range(REACH):
            i = block(slow, k)
            image_row(i, forward(s, i, 0, slots))
        for k in range(REACH):
            i = block(fast, k)
            image_row(i, partial[k] + forward(s, i, *inner(fast, k)))
        for i in middle:
            image_row(i, forward(s, i, 0, slots))

        @pl.when(g == last_pair)
        def _():
            gram(OUTER - 1, SIZE - 1, s)

        for k in range(REACH):
            adjoint(s, block(slow, k), *edge(slow, k))
        hand_over(slow)
        for k in range(REACH):
            adjoint(s, block(slow, k), *inner(slow, k))
            adjoint(s, block(fast, k), 0, slots)
        for i in middle:
            adjoint(s, i, 0, slots)
        def own_part(i):
            total = None
            for r in range(nblk):
                term = parts[source(r, i - r)]
                total = term if total is None else total + term
            acc[s, i] = total

        def own_parts(side):
            for k in range(REACH):
                own_part(block(side, k))

            @pl.when(g < last_pair)
            def _():
                for k in range(REACH):
                    acc_copy(1 - slot, s, side, k, 1 - side).start()

        own_parts(slow)
        hand_over(fast)
        own_parts(fast)
        for i in middle:
            own_part(i)

        @pl.when(g < last_pair)
        def _():
            gram(o, tl, s)
            gram(o, tl + 1, s)

        point(streams * g + s)

    grow[...] = jnp.zeros_like(grow)
    parts[nblk * slots] = jnp.zeros((width, tile), F32)
    scale[...] = jnp.ones_like(scale)
    give[...] = jnp.zeros_like(give)
    got[0] = jnp.zeros_like(got[0])

    def turn(i):
        load_start(i).wait()
        value = first[i].T
        for s in range(streams):
            acc[s, i] = value[s * width : (s + 1) * width]

    for k in range(REACH):
        turn(block(slow, k))
    pl.semaphore_wait(barrier, len(others))
    for s in range(streams):
        for k in range(REACH):
            acc_copy(0, s, slow, k, 1 - slow).start()
    for k in range(REACH):
        turn(block(fast, k))
    for s in range(streams):
        for k in range(REACH):
            acc_copy(0, s, fast, k, 1 - fast).start()
    for i in middle:
        turn(i)
    load_tiles.wait()
    load_offs.wait()

    def prepare(i, carry):
        for s in range(slots):
            value = raw[i, sorted_slot(i, s)[0]]
            high, low = halves(value)
            adj_high[i, s] = high
            adj_low[i, s] = low
            high, low = halves(value.T)
            fwd_high[i, pl.ds(s * tile, tile)] = high
            fwd_low[i, pl.ds(s * tile, tile)] = low
        return carry

    lax.fori_loop(0, nblk, prepare, 0)

    def pair(g, carry):
        def stream(s, c):
            phase(g, s)
            return c

        return lax.fori_loop(0, streams, stream, carry)

    lax.fori_loop(0, last_pair + 1, pair, 0)

    def last(s):
        slot = (last_pair + 1) % 2
        for side in (fast, slow):
            for k in range(REACH):
                i = block(side, k)
                part_copy(slot, s, side, k, side).wait()
                ends[s, i] = acc[s, i] + got[slot, s, side, k]
        for i in middle:
            ends[s, i] = acc[s, i]

    for s in range(streams - 1):
        last(s)
    advance(OUTER - 1, 2, 0)
    advance(OUTER - 1, 3, 0)
    last(streams - 1)
    for kind in (2, 3, 1, 0):
        taken[OUTER - 1, kind] = max(taken[OUTER - 1, kind], 1)
        finish(OUTER - 1, kind)
    if OUTER > 1:
        for kind in range(1, len(GROUPS)):
            finish(0, kind)


def closing(total_rows, totals, ends, gram_ref, final_ref):
    streams, nblk, _, _ = ends.shape
    true = jnp.ones((1, totals.shape[2]), F32)
    for o in range(OUTER):
        for a in range(SIZE):
            for b in range(SIZE):
                x, y = a % DEPTH, b % DEPTH
                if a // DEPTH == b // DEPTH:
                    row = FIRST[x + y + a // DEPTH]
                else:
                    x, y = (x, y) if a < DEPTH else (y, x)
                    row = FIRST[2 * y + 1] + 1 + x if x <= y else FIRST[2 * x] + 1 + y
                value = totals[o, row : row + 1, :] / total_rows
                gram_ref[o, pl.ds(a * SIZE + b, 1), :] = value * true * true
        row = FIRST[SIZE - 1]
        corner = totals[o, row : row + 1, :] / total_rows * true * true
        norm = true / jnp.sqrt(corner + 0.25)
        if o < OUTER - 1:
            true = norm / provisional(totals, o, total_rows)
    for i in range(nblk):
        value = jnp.concatenate([ends[s, i] for s in range(streams)], axis=0)
        final_ref[i] = value.T * norm


def on_device(tiles, offsets, start):
    n = lax.axis_size("blk")
    levels = n.bit_length() - 1
    assert n == 1 << levels
    bits = [[0, 3, 4], [1, 2]] + [[b, b + 1] for b in range(5, levels, 2)]
    stages = [kept for group in bits if (kept := [b for b in group if b < levels])]
    nblk, slots, tile, _ = tiles.shape
    rows, probes = start.shape
    assert nblk >= 2 * REACH and slots >= REACH and OUTER == 2
    streams = STREAMS
    width = probes // streams
    dma = pltpu.SemaphoreType.DMA
    wide = (nblk, slots * tile, tile)
    square = (nblk, slots, tile, tile)
    whole = pl.BlockSpec(memory_space=pltpu.VMEM)
    operands = (offsets, tiles, start.reshape(nblk, tile, probes))
    totals, ends = pl.pallas_call(
        functools.partial(kernel, n, stages, float(rows * n)),
        out_shape=(
            pltpu.VMEM((OUTER, 32, probes), F32),
            pltpu.VMEM((streams, nblk, width, tile), F32),
        ),
        in_specs=[
            pl.BlockSpec(memory_space=pl.ANY),
            pl.BlockSpec(memory_space=pl.ANY),
            pl.BlockSpec(memory_space=pl.ANY),
        ],
        out_specs=(whole, whole),
        scratch_shapes=[
            pltpu.SMEM(offsets.shape, jnp.int32),
            pltpu.VMEM(tiles.shape, F32),
            pltpu.VMEM((nblk, tile, probes), F32),
            pltpu.VMEM(wide, BF16),
            pltpu.VMEM(wide, BF16),
            pltpu.VMEM(square, BF16),
            pltpu.VMEM(square, BF16),
            pltpu.VMEM((streams, OUTER * SIZE, nblk, width, tile), F32),
            pltpu.VMEM((streams, nblk + 2 * REACH, 2 * width, tile), BF16),
            pltpu.VMEM((streams, nblk, 2 * width, tile), BF16),
            pltpu.VMEM((nblk * slots + 1, width, tile), F32),
            pltpu.VMEM((streams, nblk, width, tile), F32),
            pltpu.VMEM((2, streams, 2, REACH, width, tile), F32),
            pltpu.VMEM((streams, 2, REACH, width, tile), F32),
            pltpu.VMEM((2, streams, 2, REACH, width, tile), F32),
            pltpu.VMEM((2, streams, width, tile), F32),
            pltpu.VMEM((2, 1 + DEPTH, streams, width, 128), F32),
            pltpu.VMEM((OUTER, 32, probes), F32),
        ]
        + [pltpu.VMEM((OUTER, len(stages), 8, count, probes), F32) for _, count in GROUPS]
        + [
            dma((nblk,)),
            dma((2,)),
            dma((2, streams, 2, REACH)),
            dma((2, streams, 2, REACH)),
            dma((2, streams, 2, REACH)),
            dma((2, streams, 2, REACH)),
            dma((OUTER, len(GROUPS), len(stages), 7)),
            dma((OUTER, len(GROUPS), len(stages), 7)),
        ],
        compiler_params=pltpu.CompilerParams(
            collective_id=0, has_side_effects=True, vmem_limit_bytes=48 << 20
        ),
    )(*[pltpu.with_memory_space_constraint(x, pltpu.HBM) for x in operands])
    grams, final = pl.pallas_call(
        functools.partial(closing, float(rows * n)),
        out_shape=(
            jax.ShapeDtypeStruct((OUTER, SIZE * SIZE, probes), F32),
            jax.ShapeDtypeStruct((nblk, tile, probes), F32),
        ),
        in_specs=[whole, whole],
        out_specs=(whole, whole),
        compiler_params=pltpu.CompilerParams(vmem_limit_bytes=8 << 20),
    )(totals, ends)
    return grams.reshape(OUTER, SIZE, SIZE, probes), final.reshape(rows, probes)


def solution(mesh):
    placed = (P("blk", None, None, None), P("blk", None), P("blk", None))
    return jax.shard_map(
        on_device, mesh=mesh, in_specs=placed, out_specs=(P(), P("blk", None)), check_vma=False
    )
```
